32 devices in a mesh: grp: 2 (over y), seq: 8 (over z, x), head: 2 (over core).
Axes of the slice: x: 2, y: 2, z: 4, core: 2. Of those that a mesh axis runs over, the one named last changes fastest.
Arguments:
- key_cache: bfloat16 [4, 64, 128, 1024], P('grp', ('seq', 'head')), parts along dimension 0, may hold values from -160 to 160, as said below
- value_cache: bfloat16 [4, 64, 128, 1024], P('grp', ('seq', 'head')), parts along dimension 0, may hold values from -16 to 16, as said below
- query: bfloat16 [4, 4096], P('grp', 'head'), parts along dimension 0, may hold values from -48 to 48, as said below
- lengths: int32 [4], P('grp'), parts along dimension 0, may hold values from 128 to 8192, as said below
- block_map: int32 [4, 64], P('grp'), parts along dimension 0, may hold values from 0 to 63, each once within a row
Outputs:
- attended: bfloat16 [4, 4096], P('grp', 'head'), parts along dimension 0
The draws below stay inside these ranges and needn't reach their ends.
There are 2 independent parts, one for each index of `grp`. The reference program is written for one: setup_inputs(seed, part) draws one part's arguments, and reference() takes and returns one part's arrays. A program takes and returns all parts, laid end to end along the dimension named above; each array names one. Nothing has to cross between parts.
Inputs may be any that keep to these rules, and one draw needn't show every extreme that they name: `lengths`: every length is a multiple of 128; in every draw some request has length 8192. `key_cache`: finite entries, drawn afresh for every request, block, token and channel. `value_cache`: finite entries, drawn afresh for every request, block, token and channel. `query`: finite entries, drawn afresh for every request, head and channel.
All inputs are finite; a program needn't handle non-finite values.
Results may differ from the reference program's by a relative error of at most 0.0055.
Values may be sent and summed in bfloat16 or wider, within the bound.
A program may use at most 64 MiB of HBM per device.

```python
import jax
import jax.numpy as jnp
from jax import lax

QH = 32
KVH = 8
HD = 128
BLK = 128
BATCH = 2
NBLK = 64


def layout_terms(key):
    first_key, second_key, third_key = jax.random.split(jax.random.fold_in(key, 11), 3)
    direction = jax.random.normal(first_key, (KVH, HD), jnp.float32)
    direction = direction / jnp.sqrt(jnp.sum(direction * direction, axis=1, keepdims=True))
    coeffs = jax.random.uniform(second_key, (BATCH, NBLK, KVH), jnp.float32, -1.5, 1.5)
    return (direction, coeffs)


def draw_key_cache(key, part):
    direction, coeffs = layout_terms(key)
    shape = (BATCH, NBLK, BLK, KVH, HD)
    noise = jax.random.normal(jax.random.fold_in(key, 21), shape, jnp.float32)
    keys_full = noise + coeffs[:, :, None, :, None] * direction[None, None, None, :, :]
    return keys_full.reshape(BATCH, NBLK, BLK, KVH * HD).astype(jnp.bfloat16)


def draw_value_cache(key, part):
    means = jax.random.normal(jax.random.fold_in(key, 31), (BATCH, NBLK, KVH * HD), jnp.float32)
    noise = 0.5 * jax.random.normal(jax.random.fold_in(key, 32), (BATCH, NBLK, BLK, KVH * HD), jnp.float32)
    return (noise + means[:, :, None, :]).astype(jnp.bfloat16)


def draw_query(key, part):
    direction, coeffs = layout_terms(key)
    noise = jax.random.normal(jax.random.fold_in(key, 41), (BATCH, KVH, QH // KVH, HD), jnp.float32)
    full = noise + 2.0 * HD ** 0.5 * direction[None, :, None, :]
    return full.reshape(BATCH, QH * HD).astype(jnp.bfloat16)


def draw_lengths(key, part):
    first_key, second_key = jax.random.split(jax.random.fold_in(key, 51))
    counts = jax.random.randint(first_key, (BATCH,), 1, NBLK + 1)
    fullest = jax.random.randint(second_key, (), 0, BATCH)
    counts = jnp.where(jnp.arange(BATCH) == fullest, NBLK, counts)
    return (counts * BLK).astype(jnp.int32)


def setup_inputs(seed: int = 0, part: int = 0) -> dict:
    splits = jax.random.split(jax.random.key(seed), 6)
    part_splits = jax.random.split(jax.random.fold_in(splits[5], part), 6)
    key_cache = draw_key_cache(jax.random.fold_in(jax.random.fold_in(splits[5], part), 71), part)
    value_cache = draw_value_cache(jax.random.fold_in(jax.random.fold_in(splits[5], part), 71), part)
    query = draw_query(jax.random.fold_in(jax.random.fold_in(splits[5], part), 71), part)
    lengths = draw_lengths(jax.random.fold_in(jax.random.fold_in(splits[5], part), 71), part)
    block_map = jax.vmap(lambda own: jax.random.permutation(own, NBLK))(jax.random.split(part_splits[4], BATCH)).reshape((BATCH, NBLK)).astype(jnp.int32)
    return dict(key_cache=key_cache, value_cache=value_cache, query=query, lengths=lengths, block_map=block_map)


def reference(key_cache, value_cache, query, lengths, block_map):
    key_rows = key_cache.reshape(BATCH, NBLK * BLK, KVH, HD)
    value_rows = value_cache.reshape(BATCH, NBLK * BLK, KVH, HD)
    live_blocks = block_map < (lengths // BLK)[:, None]
    live_tokens = jnp.repeat(live_blocks, BLK, axis=1)[:, None, :]
    queries = query.reshape(BATCH, KVH, QH // KVH, HD).astype(jnp.float32)
    score_scale = 1.0 / (HD ** 0.5)

    def one_group(group):
        key_portion = key_rows[:, :, group, :].astype(jnp.float32)
        value_portion = value_rows[:, :, group, :].astype(jnp.float32)
        query_portion = queries[:, group]
        logit_scores = jnp.einsum("rcy,rly->rcl", query_portion, key_portion, precision=lax.Precision.HIGHEST) * score_scale
        row_top = jnp.max(jnp.where(live_tokens, logit_scores, jnp.float32(-1e30)), axis=-1)
        expo = jnp.where(live_tokens, jnp.exp(logit_scores - row_top[..., None]), jnp.float32(0.0))
        total = jnp.sum(expo, axis=-1)
        rounded_scores = lax.optimization_barrier(expo.astype(jnp.bfloat16)).astype(jnp.float32)
        summed_values = jnp.einsum("wog,wgn->won", rounded_scores, value_portion, precision=lax.Precision.HIGHEST)
        return summed_values / total[..., None]

    outputs = lax.map(one_group, jnp.arange(KVH, dtype=jnp.int32))
    outputs = jnp.transpose(outputs, (1, 0, 2, 3)).reshape(BATCH, QH * HD)
    return outputs.astype(jnp.bfloat16)
```

```python
import functools

import jax
import jax.numpy as jnp
from jax import lax
from jax.experimental import pallas as pl
from jax.experimental.pallas import tpu as pltpu
from jax.sharding import PartitionSpec as P

QH = 32
KVH = 8
HD = 128
BLK = 128
REP = QH // KVH
MESH = pl.DeviceIdType.MESH
NEG = -1e30


def kernel(
    n_seq, n_head,
    lengths, block_map, q_ref, k_hbm, v_hbm, out_ref,
    k_buf, v_buf, q_mate, num_send, stat_send, num_recv, stat_recv,
    kv_sem, q_sem, nsend_sem, nrecv_sem, ssend_sem, srecv_sem,
):
    seq = lax.axis_index("seq")
    head = lax.axis_index("head")
    batch, slots = k_hbm.shape[0], k_hbm.shape[1]
    width = k_hbm.shape[3] // n_head
    groups = width // HD
    rows_b = groups * REP
    rows = batch * rows_b
    tokens = slots * BLK
    me = seq * n_head + head
    n_all = n_seq * n_head
    small = n_all <= 16

    def loop(lo, hi, body):
        if small:
            for i in range(lo, hi):
                body(i)
        else:
            def step(i, carry):
                body(i)
                return carry
            lax.fori_loop(lo, hi, step, 0)

    def peer(step):
        return lax.rem(me + step, n_all)

    def place(device):
        return {"seq": device // n_head, "head": lax.rem(device, n_head)}

    barrier = pltpu.get_barrier_semaphore()

    def greet(step):
        pl.semaphore_signal(barrier, inc=1, device_id=place(peer(step)), device_id_type=MESH)

    loop(1, n_all, greet)

    def load(half, which, b):
        owner = lax.rem(head + half, n_head)
        source, target = ((k_hbm, k_buf), (v_hbm, v_buf))[which]
        lanes = pl.ds(pl.multiple_of(owner * width, width), width)
        return pltpu.make_async_copy(
            source.at[b, :, :, lanes], target.at[half, b], kv_sem.at[half, which, b]
        )

    for half in range(n_head):
        for which in range(2):
            for b in range(batch):
                load(half, which, b).start()

    def live_of(b):
        flags = []
        for j in range(slots):
            here = block_map[b, me * slots + j] * BLK < lengths[b]
            flags.append(jnp.broadcast_to(jnp.where(here, 1.0, 0.0), (rows_b, BLK)))
        return jnp.concatenate(flags, axis=1) > 0.5

    def diagonal(q):
        lifted = q.astype(jnp.float32).reshape(rows, HD)
        wide = jnp.concatenate([lifted] * groups, axis=1)
        row_group = lax.rem(lax.broadcasted_iota(jnp.int32, wide.shape, 0), rows_b) // REP
        lane_group = lax.broadcasted_iota(jnp.int32, wide.shape, 1) // HD
        return jnp.where(row_group == lane_group, wide, 0.0).astype(jnp.bfloat16)

    live = [live_of(b) for b in range(batch)]

    def attend(half, q):
        spread = diagonal(q)
        expos, tops, totals, nums = [], [], [], []
        for b in range(batch):
            load(half, 0, b).wait()
            keys = k_buf[half, b].reshape(tokens, width)
            scores = lax.dot_general(
                spread[b * rows_b:(b + 1) * rows_b], keys, (((1,), (1,)), ((), ())),
                preferred_element_type=jnp.float32,
            ) * (1.0 / HD**0.5)
            scores = jnp.where(live[b], scores, NEG)
            top = jnp.max(scores, axis=1, keepdims=True)
            expo = jnp.where(live[b], jnp.exp(scores - top), 0.0)
            tops.append(top)
            totals.append(jnp.sum(expo, axis=1, keepdims=True))
            expos.append(expo.astype(jnp.bfloat16))
        for b in range(batch):
            load(half, 1, b).wait()
            values = v_buf[half, b].reshape(tokens, width)
            full = jnp.dot(expos[b], values, preferred_element_type=jnp.float32)
            row_group = lax.broadcasted_iota(jnp.int32, (rows_b, HD), 0) // REP
            part = jnp.zeros((rows_b, HD), jnp.float32)
            for g in range(groups):
                part = jnp.where(row_group == g, full[:, g * HD:(g + 1) * HD], part)
            nums.append(part)
        column = jnp.concatenate(tops + totals + [jnp.zeros((HD - 2 * rows, 1), jnp.float32)], axis=0)
        record = jnp.transpose(jnp.broadcast_to(column, (HD, HD)))[0:1]
        return jnp.concatenate(nums, axis=0), record

    def copies(device, half, slot_of):
        return (
            pltpu.make_async_remote_copy(
                src_ref=stat_send.at[pl.ds(half, 1)], dst_ref=stat_recv.at[pl.ds(slot_of, 1)],
                send_sem=ssend_sem.at[device], recv_sem=srecv_sem.at[slot_of],
                device_id=place(device), device_id_type=MESH,
            ),
            pltpu.make_async_remote_copy(
                src_ref=num_send.at[half], dst_ref=num_recv.at[slot_of],
                send_sem=nsend_sem.at[device], recv_sem=nrecv_sem.at[slot_of],
                device_id=place(device), device_id_type=MESH,
            ),
        )

    def send_half(half):
        def one(d):
            target_seq = lax.rem(seq + d, n_seq)
            target = target_seq * n_head + lax.rem(head + half, n_head)
            for copy in copies(target, half, me):
                copy.start()
        loop(0 if half else 1, n_seq, one)

    pl.semaphore_wait(barrier, n_all - 1)
    q_copy = pltpu.make_async_remote_copy(
        src_ref=q_ref, dst_ref=q_mate, send_sem=q_sem.at[0], recv_sem=q_sem.at[1],
        device_id={"head": lax.rem(head + 1, n_head)}, device_id_type=MESH,
    )
    q_copy.start()
    own_num, own_stat = attend(0, q_ref[...])
    num_send[0] = own_num.astype(jnp.bfloat16)
    stat_send[0:1] = own_stat
    send_half(0)
    q_copy.wait()
    mate_num, mate_stat = attend(1, q_mate[...])
    num_send[1] = mate_num.astype(jnp.bfloat16)
    stat_send[1:2] = mate_stat
    send_half(1)

    stat_recv[pl.ds(me, 1)] = own_stat
    num_recv[me] = own_num.astype(jnp.bfloat16)

    def arrive_stat(step):
        copies(peer(step), 0, peer(step))[0].wait_recv()

    def arrive_num(step):
        copies(peer(step), 0, peer(step))[1].wait_recv()

    loop(1, n_all, arrive_stat)
    stats = stat_recv[...]
    top = stats[:, :rows]
    total = stats[:, rows:2 * rows]
    factor = jnp.exp(top - jnp.max(top, axis=0, keepdims=True))
    share = factor / jnp.sum(factor * total, axis=0, keepdims=True)
    share_columns = jnp.transpose(jnp.concatenate(
        [share, jnp.zeros((n_all, HD - rows), jnp.float32)], axis=1))[:rows]
    loop(1, n_all, arrive_num)
    result = jnp.zeros((rows, HD), jnp.float32)
    for s in range(n_all):
        result = result + share_columns[:, s:s + 1] * num_recv[s].astype(jnp.float32)
    out_ref[...] = result.astype(out_ref.dtype)

    def sent(step):
        for copy in copies(peer(step), 0, me):
            copy.wait_send()

    loop(1, n_all, sent)


def solution(mesh):
    n_seq, n_head = mesh.shape["seq"], mesh.shape["head"]
    n_all = n_seq * n_head

    def on_device(key_cache, value_cache, query, lengths, block_map):
        batch, slots, _, channels = key_cache.shape
        width = channels // n_head
        rows = batch * (width // HD) * REP
        dma = pltpu.SemaphoreType.DMA
        result = pl.pallas_call(
            functools.partial(kernel, n_seq, n_head),
            out_shape=jax.ShapeDtypeStruct((rows, HD), jnp.bfloat16),
            in_specs=[
                pl.BlockSpec(memory_space=pltpu.SMEM),
                pl.BlockSpec(memory_space=pltpu.SMEM),
                pl.BlockSpec(memory_space=pltpu.VMEM),
                pl.BlockSpec(memory_space=pl.ANY),
                pl.BlockSpec(memory_space=pl.ANY),
            ],
            out_specs=pl.BlockSpec(memory_space=pltpu.VMEM),
            scratch_shapes=[
                pltpu.VMEM((n_head, batch, slots, BLK, width), jnp.bfloat16),
                pltpu.VMEM((n_head, batch, slots, BLK, width), jnp.bfloat16),
                pltpu.VMEM(query.shape, jnp.bfloat16),
                pltpu.VMEM((n_head, rows, HD), jnp.bfloat16),
                pltpu.VMEM((n_head, HD), jnp.float32),
                pltpu.VMEM((n_all, rows, HD), jnp.bfloat16),
                pltpu.VMEM((n_all, HD), jnp.float32),
                dma((n_head, 2, batch)),
                dma((2,)),
                dma((n_all,)),
                dma((n_all,)),
                dma((n_all,)),
                dma((n_all,)),
            ],
            compiler_params=pltpu.CompilerParams(collective_id=0, has_side_effects=True),
        )(lengths, block_map, query, key_cache, value_cache)
        return result.reshape(query.shape)

    placed = (
        P("grp", ("seq", "head"), None, None),
        P("grp", ("seq", "head"), None, None),
        P("grp", "head"),
        P("grp"),
        P("grp", None),
    )
    return jax.shard_map(
        on_device, mesh=mesh, in_specs=placed, out_specs=P("grp", "head"), check_vma=False
    )
```

```python
import functools

import jax
import jax.numpy as jnp
from jax import lax
from jax.experimental import pallas as pl
from jax.experimental.pallas import tpu as pltpu
from jax.sharding import PartitionSpec as P

QH = 32
KVH = 8
HD = 128
BLK = 128
REP = QH // KVH
MESH = pl.DeviceIdType.MESH
NEG = -1e30


def kernel(
    n_seq, n_head, n_plane,
    lengths_hbm, map_hbm, q_hbm, k_hbm, v_hbm, out_ref,
    lengths, block_map, q_own, q_mate, k_buf, v_buf,
    num_send, stat_send, num_recv, stat_recv, num_send2, stat_send2, num_recv2, stat_recv2,
    small_sem, q_sem, kv_sem, num_sem, stat_sem, num_sem2, stat_sem2, up_sem, down_sem,
):
    seq = lax.axis_index("seq")
    head = lax.axis_index("head")
    batch, slots = k_hbm.shape[0], k_hbm.shape[1]
    width = k_hbm.shape[3] // n_head
    groups = width // HD
    rows_b = groups * REP
    rows = batch * rows_b
    tokens = slots * BLK
    n_line = n_seq // n_plane
    line, across = seq // n_plane, lax.rem(seq, n_plane)
    members = n_plane * n_head
    spot = across * n_head + head
    me = seq * n_head + head

    barrier = pltpu.get_barrier_semaphore()
    below, above = line > 0, line < n_line - 1

    def signal(sem, device):
        pl.semaphore_signal(sem, inc=1, device_id=device, device_id_type=MESH)

    @pl.when(below)
    def _():
        signal(barrier, {"seq": seq - n_plane})

    @pl.when(above)
    def _():
        signal(barrier, {"seq": seq + n_plane})

    for step in range(1, members):
        other = lax.rem(spot + step, members)
        signal(barrier, {"seq": line * n_plane + other // n_head, "head": lax.rem(other, n_head)})

    q_load = pltpu.make_async_copy(q_hbm, q_own, small_sem.at[0])
    q_load.start()
    length_load = pltpu.make_async_copy(lengths_hbm, lengths, small_sem.at[1])
    length_load.start()
    map_load = pltpu.make_async_copy(map_hbm, block_map, small_sem.at[2])
    map_load.start()

    def load(half, which, b):
        owner = lax.rem(head + half, n_head)
        source, target = ((k_hbm, k_buf), (v_hbm, v_buf))[which]
        lanes = pl.ds(pl.multiple_of(owner * width, width), width)
        return pltpu.make_async_copy(
            source.at[b, :, :, lanes], target.at[half, b], kv_sem.at[half, which, b]
        )

    for half in range(n_head):
        for which in range(2):
            for b in range(batch):
                load(half, which, b).start()

    length_load.wait()
    map_load.wait()
    q_load.wait()
    contacts = members - 1 + below.astype(jnp.int32) + above.astype(jnp.int32)
    pl.semaphore_wait(barrier, contacts)
    q_copy = pltpu.make_async_remote_copy(
        src_ref=q_own, dst_ref=q_mate, send_sem=q_sem.at[0], recv_sem=q_sem.at[1],
        device_id={"head": lax.rem(head + 1, n_head)}, device_id_type=MESH,
    )
    q_copy.start()

    @pl.when(above)
    def _():
        signal(up_sem, {"seq": seq + n_plane})

    @pl.when(below)
    def _():
        signal(down_sem, {"seq": seq - n_plane})

    def relay(lo, hi):
        for step in range(lo, hi):
            @pl.when(line >= step)
            def _():
                pl.semaphore_wait(up_sem, 1)

            @pl.when((line >= step) & above)
            def _():
                signal(up_sem, {"seq": seq + n_plane})

            @pl.when(n_line - 1 - line >= step)
            def _():
                pl.semaphore_wait(down_sem, 1)

            @pl.when((n_line - 1 - line >= step) & below)
            def _():
                signal(down_sem, {"seq": seq - n_plane})

    def live_of(b):
        flags = []
        for j in range(slots):
            here = block_map[b, me * slots + j] * BLK < lengths[b]
            flags.append(jnp.broadcast_to(jnp.where(here, 1.0, 0.0), (rows_b, BLK)))
        return jnp.concatenate(flags, axis=1) > 0.5

    def diagonal(q):
        lifted = q.astype(jnp.float32).reshape(rows, HD)
        wide = jnp.concatenate([lifted] * groups, axis=1)
        row_group = lax.rem(lax.broadcasted_iota(jnp.int32, wide.shape, 0), rows_b) // REP
        lane_group = lax.broadcasted_iota(jnp.int32, wide.shape, 1) // HD
        return jnp.where(row_group == lane_group, wide, 0.0).astype(jnp.bfloat16)

    live = [live_of(b) for b in range(batch)]

    def attend(half, q):
        spread = diagonal(q)
        expos, tops, totals, nums = [], [], [], []
        for b in range(batch):
            load(half, 0, b).wait()
            keys = k_buf[half, b].reshape(tokens, width)
            scores = lax.dot_general(
                spread[b * rows_b:(b + 1) * rows_b], keys, (((1,), (1,)), ((), ())),
                preferred_element_type=jnp.float32,
            ) * (1.0 / HD**0.5)
            scores = jnp.where(live[b], scores, NEG)
            top = jnp.max(scores, axis=1, keepdims=True)
            expo = jnp.where(live[b], jnp.exp(scores - top), 0.0)
            tops.append(top)
            totals.append(jnp.sum(expo, axis=1, keepdims=True))
            expos.append(expo.astype(jnp.bfloat16))
        for b in range(batch):
            load(half, 1, b).wait()
            values = v_buf[half, b].reshape(tokens, width)
            full = jnp.dot(expos[b], values, preferred_element_type=jnp.float32)
            row_group = lax.broadcasted_iota(jnp.int32, (rows_b, HD), 0) // REP
            part = jnp.zeros((rows_b, HD), jnp.float32)
            for g in range(groups):
                part = jnp.where(row_group == g, full[:, g * HD:(g + 1) * HD], part)
            nums.append(part)
        column = jnp.concatenate(tops + totals + [jnp.zeros((HD - 2 * rows, 1), jnp.float32)], axis=0)
        record = jnp.transpose(jnp.broadcast_to(column, (HD, HD)))[0:1]
        return jnp.concatenate(nums, axis=0), record

    def hand(source, target, sems, index, slot, device):
        return pltpu.make_async_remote_copy(
            src_ref=source, dst_ref=target, send_sem=sems.at[0, index], recv_sem=sems.at[1, slot],
            device_id=device, device_id_type=MESH,
        )

    def plane_hand(kind, half, other, slot):
        device = {"seq": line * n_plane + other // n_head, "head": lax.rem(other, n_head)}
        if kind == 0:
            return hand(stat_send.at[pl.ds(half, 1)], stat_recv.at[pl.ds(slot, 1)], stat_sem, other, slot, device)
        return hand(num_send.at[half], num_recv.at[slot], num_sem, other, slot, device)

    def line_hand(kind, other, slot):
        device = {"seq": other * n_plane + across}
        if kind == 0:
            return hand(stat_send2, stat_recv2.at[pl.ds(slot, 1)], stat_sem2, other, slot, device)
        return hand(num_send2, num_recv2.at[slot], num_sem2, other, slot, device)

    def plane_send(half):
        for kind in range(2):
            for d in range(0 if half else 1, n_plane):
                other = lax.rem(across + d, n_plane) * n_head + lax.rem(head + half, n_head)
                plane_hand(kind, half, other, spot).start()

    def merged(stats):
        top, total = stats[:, :rows], stats[:, rows:2 * rows]
        best = jnp.max(top, axis=0, keepdims=True)
        factor = jnp.exp(top - best)
        whole = jnp.sum(factor * total, axis=0, keepdims=True)
        return best, factor, whole

    def columns(factor):
        count = factor.shape[0]
        padded = -count % 8
        tall = factor if not padded else jnp.concatenate(
            [factor, jnp.zeros((padded, rows), jnp.float32)], axis=0)
        return jnp.transpose(jnp.concatenate(
            [tall, jnp.zeros((tall.shape[0], HD - rows), jnp.float32)], axis=1))[:rows]

    own_num, own_stat = attend(0, q_own[...])
    num_send[0] = own_num.astype(jnp.bfloat16)
    stat_send[0:1] = own_stat
    plane_send(0)
    relay(1, 2)
    q_copy.wait()
    mate_num, mate_stat = attend(1, q_mate[...])
    num_send[1] = mate_num.astype(jnp.bfloat16)
    stat_send[1:2] = mate_stat
    plane_send(1)
    relay(2, n_line)

    stat_recv[pl.ds(spot, 1)] = own_stat
    num_recv[spot] = own_num.astype(jnp.bfloat16)
    for kind in range(2):
        for step in range(1, members):
            other = lax.rem(spot + step, members)
            plane_hand(kind, 0, other, other).wait_recv()
    best, factor, whole = merged(stat_recv[...])
    share = columns(factor)
    plane_num = jnp.zeros((rows, HD), jnp.float32)
    for s in range(members):
        plane_num = plane_num + share[:, s:s + 1] * num_recv[s].astype(jnp.float32)
    plane_stat = jnp.concatenate(
        [best, whole, jnp.zeros((1, HD - 2 * rows), jnp.float32)], axis=1)
    stat_send2[...] = plane_stat
    num_send2[...] = plane_num.astype(jnp.bfloat16)
    for kind in range(2):
        for step in range(1, n_line):
            line_hand(kind, lax.rem(line + step, n_line), line).start()
    stat_recv2[pl.ds(line, 1)] = plane_stat
    num_recv2[line] = plane_num.astype(jnp.bfloat16)
    for kind in range(2):
        for step in range(1, n_line):
            other = lax.rem(line + step, n_line)
            line_hand(kind, other, other).wait_recv()
    best, factor, whole = merged(stat_recv2[...])
    share = columns(factor / whole)
    result = jnp.zeros((rows, HD), jnp.float32)
    for s in range(n_line):
        result = result + share[:, s:s + 1] * num_recv2[s].astype(jnp.float32)
    out_ref[...] = result.reshape(batch, rows_b * HD).astype(out_ref.dtype)

    for kind in range(2):
        for step in range(1, members):
            other = lax.rem(spot + step, members)
            plane_hand(kind, 0, other, spot).wait_send()
        for step in range(1, n_line):
            line_hand(kind, lax.rem(line + step, n_line), line).wait_send()


def plane_of(n_seq):
    size = 1
    while (size + 1) ** 2 <= n_seq:
        size += 1
    while n_seq % size:
        size -= 1
    return size


def solution(mesh):
    n_seq, n_head = mesh.shape["seq"], mesh.shape["head"]
    n_plane = plane_of(n_seq)
    n_line, members = n_seq // n_plane, n_plane * n_head

    def on_device(key_cache, value_cache, query, lengths, block_map):
        batch, slots, _, channels = key_cache.shape
        width = channels // n_head
        rows = batch * (width // HD) * REP
        dma = pltpu.SemaphoreType.DMA
        result = pl.pallas_call(
            functools.partial(kernel, n_seq, n_head, n_plane),
            out_shape=jax.ShapeDtypeStruct(query.shape, jnp.bfloat16),
            in_specs=[pl.BlockSpec(memory_space=pl.ANY)] * 5,
            out_specs=pl.BlockSpec(memory_space=pltpu.VMEM),
            scratch_shapes=[
                pltpu.SMEM(lengths.shape, jnp.int32),
                pltpu.SMEM(block_map.shape, jnp.int32),
                pltpu.VMEM(query.shape, jnp.bfloat16),
                pltpu.VMEM(query.shape, jnp.bfloat16),
                pltpu.VMEM((n_head, batch, slots, BLK, width), jnp.bfloat16),
                pltpu.VMEM((n_head, batch, slots, BLK, width), jnp.bfloat16),
                pltpu.VMEM((n_head, rows, HD), jnp.bfloat16),
                pltpu.VMEM((n_head, HD), jnp.float32),
                pltpu.VMEM((members, rows, HD), jnp.bfloat16),
                pltpu.VMEM((members, HD), jnp.float32),
                pltpu.VMEM((rows, HD), jnp.bfloat16),
                pltpu.VMEM((1, HD), jnp.float32),
                pltpu.VMEM((n_line, rows, HD), jnp.bfloat16),
                pltpu.VMEM((n_line, HD), jnp.float32),
                dma((3,)),
                dma((2,)),
                dma((n_head, 2, batch)),
                dma((2, members)),
                dma((2, members)),
                dma((2, n_line)),
                dma((2, n_line)),
                pltpu.SemaphoreType.REGULAR,
                pltpu.SemaphoreType.REGULAR,
            ],
            compiler_params=pltpu.CompilerParams(collective_id=0, has_side_effects=True),
        )(lengths, block_map, query, key_cache, value_cache)
        return result

    placed = (
        P("grp", ("seq", "head"), None, None),
        P("grp", ("seq", "head"), None, None),
        P("grp", "head"),
        P("grp"),
        P("grp", None),
    )
    return jax.shard_map(
        on_device, mesh=mesh, in_specs=placed, out_specs=P("grp", "head"), check_vma=False
    )
```

```python
import functools

import jax
import jax.numpy as jnp
from jax import lax
from jax.experimental import pallas as pl
from jax.experimental.pallas import tpu as pltpu
from jax.sharding import PartitionSpec as P

QH = 32
KVH = 8
HD = 128
BLK = 128
REP = QH // KVH
MESH = pl.DeviceIdType.MESH
NEG = -1e30


def kernel(
    n_seq, n_head,
    lengths_hbm, map_hbm, q_hbm, k_hbm, v_hbm, out_ref,
    lengths, block_map, q_ref, small_sem,
    k_buf, v_buf, q_mate, num_send, stat_send, num_recv, stat_recv,
    kv_sem, q_sem, nsend_sem, nrecv_sem, ssend_sem, srecv_sem,
):
    seq = lax.axis_index("seq")
    head = lax.axis_index("head")
    batch, slots = k_hbm.shape[0], k_hbm.shape[1]
    width = k_hbm.shape[3] // n_head
    groups = width // HD
    rows_b = groups * REP
    rows = batch * rows_b
    tokens = slots * BLK
    me = seq * n_head + head
    n_all = n_seq * n_head
    small = n_all <= 16

    def loop(lo, hi, body):
        if small:
            for i in range(lo, hi):
                body(i)
        else:
            def step(i, carry):
                body(i)
                return carry
            lax.fori_loop(lo, hi, step, 0)

    def peer(step):
        return lax.rem(me + step, n_all)

    def place(device):
        return {"seq": device // n_head, "head": lax.rem(device, n_head)}

    barrier = pltpu.get_barrier_semaphore()

    def greet(step):
        pl.semaphore_signal(barrier, inc=1, device_id=place(peer(step)), device_id_type=MESH)

    loop(1, n_all, greet)
    smalls = [pltpu.make_async_copy(a, b, small_sem.at[i]) for i, (a, b) in enumerate(
        ((q_hbm, q_ref), (lengths_hbm, lengths), (map_hbm, block_map)))]
    for copy in smalls:
        copy.start()

    def load(half, which, b):
        owner = lax.rem(head + half, n_head)
        source, target = ((k_hbm, k_buf), (v_hbm, v_buf))[which]
        lanes = pl.ds(pl.multiple_of(owner * width, width), width)
        return pltpu.make_async_copy(
            source.at[b, :, :, lanes], target.at[half, b], kv_sem.at[half, which, b]
        )

    for half in range(n_head):
        for which in range(2):
            for b in range(batch):
                load(half, which, b).start()

    def live_of(b):
        flags = []
        for j in range(slots):
            here = block_map[b, me * slots + j] * BLK < lengths[b]
            flags.append(jnp.broadcast_to(jnp.where(here, 1.0, 0.0), (rows_b, BLK)))
        return jnp.concatenate(flags, axis=1) > 0.5

    def diagonal(q):
        lifted = q.astype(jnp.float32).reshape(rows, HD)
        wide = jnp.concatenate([lifted] * groups, axis=1)
        row_group = lax.rem(lax.broadcasted_iota(jnp.int32, wide.shape, 0), rows_b) // REP
        lane_group = lax.broadcasted_iota(jnp.int32, wide.shape, 1) // HD
        return jnp.where(row_group == lane_group, wide, 0.0).astype(jnp.bfloat16)

    for copy in smalls:
        copy.wait()
    live = [live_of(b) for b in range(batch)]

    def attend(half, q):
        spread = diagonal(q)
        expos, tops, totals, nums = [], [], [], []
        for b in range(batch):
            load(half, 0, b).wait()
            keys = k_buf[half, b].reshape(tokens, width)
            scores = lax.dot_general(
                spread[b * rows_b:(b + 1) * rows_b], keys, (((1,), (1,)), ((), ())),
                preferred_element_type=jnp.float32,
            ) * (1.0 / HD**0.5)
            scores = jnp.where(live[b], scores, NEG)
            top = jnp.max(scores, axis=1, keepdims=True)
            expo = jnp.where(live[b], jnp.exp(scores - top), 0.0)
            tops.append(top)
            totals.append(jnp.sum(expo, axis=1, keepdims=True))
            expos.append(expo.astype(jnp.bfloat16))
        for b in range(batch):
            load(half, 1, b).wait()
            values = v_buf[half, b].reshape(tokens, width)
            full = jnp.dot(expos[b], values, preferred_element_type=jnp.float32)
            row_group = lax.broadcasted_iota(jnp.int32, (rows_b, HD), 0) // REP
            part = jnp.zeros((rows_b, HD), jnp.float32)
            for g in range(groups):
                part = jnp.where(row_group == g, full[:, g * HD:(g + 1) * HD], part)
            nums.append(part)
        column = jnp.concatenate(tops + totals + [jnp.zeros((HD - 2 * rows, 1), jnp.float32)], axis=0)
        record = jnp.transpose(jnp.broadcast_to(column, (HD, HD)))[0:1]
        return jnp.concatenate(nums, axis=0), record

    def copies(device, half, slot_of):
        return (
            pltpu.make_async_remote_copy(
                src_ref=stat_send.at[pl.ds(half, 1)], dst_ref=stat_recv.at[pl.ds(slot_of, 1)],
                send_sem=ssend_sem.at[device], recv_sem=srecv_sem.at[slot_of],
                device_id=place(device), device_id_type=MESH,
            ),
            pltpu.make_async_remote_copy(
                src_ref=num_send.at[half], dst_ref=num_recv.at[slot_of],
                send_sem=nsend_sem.at[device], recv_sem=nrecv_sem.at[slot_of],
                device_id=place(device), device_id_type=MESH,
            ),
        )

    def send_half(half):
        def one(d):
            target_seq = lax.rem(seq + d, n_seq)
            target = target_seq * n_head + lax.rem(head + half, n_head)
            for copy in copies(target, half, me):
                copy.start()
        loop(0 if half else 1, n_seq, one)

    pl.semaphore_wait(barrier, n_all - 1)
    q_copy = pltpu.make_async_remote_copy(
        src_ref=q_ref, dst_ref=q_mate, send_sem=q_sem.at[0], recv_sem=q_sem.at[1],
        device_id={"head": lax.rem(head + 1, n_head)}, device_id_type=MESH,
    )
    q_copy.start()
    own_num, own_stat = attend(0, q_ref[...])
    num_send[0] = own_num.astype(jnp.bfloat16)
    stat_send[0:1] = own_stat
    send_half(0)
    q_copy.wait()
    mate_num, mate_stat = attend(1, q_mate[...])
    num_send[1] = mate_num.astype(jnp.bfloat16)
    stat_send[1:2] = mate_stat
    send_half(1)

    stat_recv[pl.ds(me, 1)] = own_stat
    num_recv[me] = own_num.astype(jnp.bfloat16)

    def arrive_stat(step):
        copies(peer(step), 0, peer(step))[0].wait_recv()

    def arrive_num(step):
        copies(peer(step), 0, peer(step))[1].wait_recv()

    loop(1, n_all, arrive_stat)
    stats = stat_recv[...]
    top = stats[:, :rows]
    total = stats[:, rows:2 * rows]
    factor = jnp.exp(top - jnp.max(top, axis=0, keepdims=True))
    share = factor / jnp.sum(factor * total, axis=0, keepdims=True)
    share_columns = jnp.transpose(jnp.concatenate(
        [share, jnp.zeros((n_all, HD - rows), jnp.float32)], axis=1))[:rows]
    loop(1, n_all, arrive_num)
    result = jnp.zeros((rows, HD), jnp.float32)
    for s in range(n_all):
        result = result + share_columns[:, s:s + 1] * num_recv[s].astype(jnp.float32)
    out_ref[...] = result.reshape(batch, rows_b * HD).astype(out_ref.dtype)

    def sent(step):
        for copy in copies(peer(step), 0, me):
            copy.wait_send()

    loop(1, n_all, sent)


def solution(mesh):
    n_seq, n_head = mesh.shape["seq"], mesh.shape["head"]
    n_all = n_seq * n_head

    def on_device(key_cache, value_cache, query, lengths, block_map):
        batch, slots, _, channels = key_cache.shape
        width = channels // n_head
        rows = batch * (width // HD) * REP
        dma = pltpu.SemaphoreType.DMA
        result = pl.pallas_call(
            functools.partial(kernel, n_seq, n_head),
            out_shape=pltpu.VMEM(query.shape, jnp.bfloat16),
            in_specs=[
                *[pl.BlockSpec(memory_space=pl.ANY)] * 5,
            ],
            out_specs=pl.BlockSpec(memory_space=pltpu.VMEM),
            scratch_shapes=[
                pltpu.SMEM(lengths.shape, jnp.int32),
                pltpu.SMEM(block_map.shape, jnp.int32),
                pltpu.VMEM(query.shape, jnp.bfloat16),
                dma((3,)),
                pltpu.VMEM((n_head, batch, slots, BLK, width), jnp.bfloat16),
                pltpu.VMEM((n_head, batch, slots, BLK, width), jnp.bfloat16),
                pltpu.VMEM(query.shape, jnp.bfloat16),
                pltpu.VMEM((n_head, rows, HD), jnp.bfloat16),
                pltpu.VMEM((n_head, HD), jnp.float32),
                pltpu.VMEM((n_all, rows, HD), jnp.bfloat16),
                pltpu.VMEM((n_all, HD), jnp.float32),
                dma((n_head, 2, batch)),
                dma((2,)),
                dma((n_all,)),
                dma((n_all,)),
                dma((n_all,)),
                dma((n_all,)),
            ],
            compiler_params=pltpu.CompilerParams(collective_id=0, has_side_effects=True),
        )(lengths, block_map, query, key_cache, value_cache)
        return result

    placed = (
        P("grp", ("seq", "head"), None, None),
        P("grp", ("seq", "head"), None, None),
        P("grp", "head"),
        P("grp"),
        P("grp", None),
    )
    return jax.shard_map(
        on_device, mesh=mesh, in_specs=placed, out_specs=P("grp", "head"), check_vma=False
    )
```

```python
import functools

import jax
import jax.numpy as jnp
from jax import lax
from jax.experimental import pallas as pl
from jax.experimental.pallas import tpu as pltpu
from jax.sharding import PartitionSpec as P

QH = 32
KVH = 8
HD = 128
BLK = 128
REP = QH // KVH
MESH = pl.DeviceIdType.MESH
NEG = -1e30


def kernel(
    n_seq, n_head,
    lengths_hbm, map_hbm, q_hbm, k_hbm, v_hbm, out_ref,
    lengths, block_map, q_ref, small_sem,
    k_buf, v_buf, q_mate, num_send, stat_send, num_recv, stat_recv,
    kv_sem, q_sem, nsend_sem, nrecv_sem, ssend_sem, srecv_sem,
):
    seq = lax.axis_index("seq")
    head = lax.axis_index("head")
    batch, slots = k_hbm.shape[0], k_hbm.shape[1]
    width = k_hbm.shape[3] // n_head
    groups = width // HD
    rows_b = groups * REP
    rows = batch * rows_b
    tokens = slots * BLK
    me = seq * n_head + head
    n_all = n_seq * n_head
    small = n_all <= 16

    def loop(lo, hi, body):
        if small:
            for i in range(lo, hi):
                body(i)
        else:
            def step(i, carry):
                body(i)
                return carry
            lax.fori_loop(lo, hi, step, 0)

    def peer(step):
        return lax.rem(me + step, n_all)

    def place(device):
        return {"seq": device // n_head, "head": lax.rem(device, n_head)}

    barrier = pltpu.get_barrier_semaphore()

    def greet(step):
        pl.semaphore_signal(barrier, inc=1, device_id=place(peer(step)), device_id_type=MESH)

    loop(1, n_all, greet)
    smalls = [pltpu.make_async_copy(a, b, small_sem.at[i]) for i, (a, b) in enumerate(
        ((q_hbm, q_ref), (lengths_hbm, lengths), (map_hbm, block_map)))]
    for copy in smalls:
        copy.start()

    def load(half, which, b):
        owner = lax.rem(head + half, n_head)
        source, target = ((k_hbm, k_buf), (v_hbm, v_buf))[which]
        lanes = pl.ds(pl.multiple_of(owner * width, width), width)
        return pltpu.make_async_copy(
            source.at[b, :, :, lanes], target.at[half, b], kv_sem.at[half, which, b]
        )

    for half in range(n_head):
        for which in range(2):
            for b in range(batch):
                load(half, which, b).start()

    def live_of(b):
        flags = []
        for j in range(slots):
            here = block_map[b, me * slots + j] * BLK < lengths[b]
            flags.append(jnp.broadcast_to(jnp.where(here, 1.0, 0.0), (rows_b, BLK)))
        return jnp.concatenate(flags, axis=1) > 0.5

    def diagonal(q):
        lifted = q.astype(jnp.float32).reshape(rows, HD)
        wide = jnp.concatenate([lifted] * groups, axis=1)
        row_group = lax.rem(lax.broadcasted_iota(jnp.int32, wide.shape, 0), rows_b) // REP
        lane_group = lax.broadcasted_iota(jnp.int32, wide.shape, 1) // HD
        return jnp.where(row_group == lane_group, wide, 0.0).astype(jnp.bfloat16)

    for copy in smalls:
        copy.wait()
    live = [live_of(b) for b in range(batch)]

    def attend(half, q):
        spread = diagonal(q)
        expos, tops, totals, nums = [], [], [], []
        for b in range(batch):
            load(half, 0, b).wait()
        for b in range(batch):
            keys = k_buf[half, b].reshape(tokens, width)
            scores = lax.dot_general(
                spread[b * rows_b:(b + 1) * rows_b], keys, (((1,), (1,)), ((), ())),
                preferred_element_type=jnp.float32,
            ) * (1.0 / HD**0.5)
            scores = jnp.where(live[b], scores, NEG)
            top = jnp.max(scores, axis=1, keepdims=True)
            expo = jnp.where(live[b], jnp.exp(scores - top), 0.0)
            tops.append(top)
            totals.append(jnp.sum(expo, axis=1, keepdims=True))
            expos.append(expo.astype(jnp.bfloat16))
        for b in range(batch):
            load(half, 1, b).wait()
        for b in range(batch):
            values = v_buf[half, b].reshape(tokens, width)
            full = jnp.dot(expos[b], values, preferred_element_type=jnp.float32)
            row_group = lax.broadcasted_iota(jnp.int32, (rows_b, HD), 0) // REP
            part = jnp.zeros((rows_b, HD), jnp.float32)
            for g in range(groups):
                part = jnp.where(row_group == g, full[:, g * HD:(g + 1) * HD], part)
            nums.append(part)
        column = jnp.concatenate(tops + totals + [jnp.zeros((HD - 2 * rows, 1), jnp.float32)], axis=0)
        record = jnp.transpose(jnp.broadcast_to(column, (HD, HD)))[0:1]
        return jnp.concatenate(nums, axis=0), record

    def copies(device, half, slot_of):
        return (
            pltpu.make_async_remote_copy(
                src_ref=stat_send.at[pl.ds(half, 1)], dst_ref=stat_recv.at[pl.ds(slot_of, 1)],
                send_sem=ssend_sem.at[device], recv_sem=srecv_sem.at[slot_of],
                device_id=place(device), device_id_type=MESH,
            ),
            pltpu.make_async_remote_copy(
                src_ref=num_send.at[half], dst_ref=num_recv.at[slot_of],
                send_sem=nsend_sem.at[device], recv_sem=nrecv_sem.at[slot_of],
                device_id=place(device), device_id_type=MESH,
            ),
        )

    def send_half(half):
        def one(d):
            target_seq = lax.rem(seq + d, n_seq)
            target = target_seq * n_head + lax.rem(head + half, n_head)
            for copy in copies(target, half, me):
                copy.start()
        loop(0 if half else 1, n_seq, one)

    pl.semaphore_wait(barrier, n_all - 1)
    q_copy = pltpu.make_async_remote_copy(
        src_ref=q_ref, dst_ref=q_mate, send_sem=q_sem.at[0], recv_sem=q_sem.at[1],
        device_id={"head": lax.rem(head + 1, n_head)}, device_id_type=MESH,
    )
    q_copy.start()
    own_num, own_stat = attend(0, q_ref[...])
    num_send[0] = own_num.astype(jnp.bfloat16)
    stat_send[0:1] = own_stat
    send_half(0)
    q_copy.wait()
    mate_num, mate_stat = attend(1, q_mate[...])
    num_send[1] = mate_num.astype(jnp.bfloat16)
    stat_send[1:2] = mate_stat
    send_half(1)

    stat_recv[pl.ds(me, 1)] = own_stat
    num_recv[me] = own_num.astype(jnp.bfloat16)

    def arrive_stat(step):
        copies(peer(step), 0, peer(step))[0].wait_recv()

    def arrive_num(step):
        copies(peer(step), 0, peer(step))[1].wait_recv()

    loop(1, n_all, arrive_stat)
    stats = stat_recv[...]
    top = stats[:, :rows]
    total = stats[:, rows:2 * rows]
    factor = jnp.exp(top - jnp.max(top, axis=0, keepdims=True))
    share = factor / jnp.sum(factor * total, axis=0, keepdims=True)
    share_columns = jnp.transpose(jnp.concatenate(
        [share, jnp.zeros((n_all, HD - rows), jnp.float32)], axis=1))[:rows]
    loop(1, n_all, arrive_num)
    result = jnp.zeros((rows, HD), jnp.float32)
    for s in range(n_all):
        result = result + share_columns[:, s:s + 1] * num_recv[s].astype(jnp.float32)
    out_ref[...] = result.reshape(batch, rows_b * HD).astype(out_ref.dtype)

    def sent(step):
        for copy in copies(peer(step), 0, me):
            copy.wait_send()

    loop(1, n_all, sent)


def solution(mesh):
    n_seq, n_head = mesh.shape["seq"], mesh.shape["head"]
    n_all = n_seq * n_head

    def on_device(key_cache, value_cache, query, lengths, block_map):
        batch, slots, _, channels = key_cache.shape
        width = channels // n_head
        rows = batch * (width // HD) * REP
        dma = pltpu.SemaphoreType.DMA
        result = pl.pallas_call(
            functools.partial(kernel, n_seq, n_head),
            out_shape=pltpu.VMEM(query.shape, jnp.bfloat16),
            in_specs=[
                *[pl.BlockSpec(memory_space=pl.ANY)] * 5,
            ],
            out_specs=pl.BlockSpec(memory_space=pltpu.VMEM),
            scratch_shapes=[
                pltpu.SMEM(lengths.shape, jnp.int32),
                pltpu.SMEM(block_map.shape, jnp.int32),
                pltpu.VMEM(query.shape, jnp.bfloat16),
                dma((3,)),
                pltpu.VMEM((n_head, batch, slots, BLK, width), jnp.bfloat16),
                pltpu.VMEM((n_head, batch, slots, BLK, width), jnp.bfloat16),
                pltpu.VMEM(query.shape, jnp.bfloat16),
                pltpu.VMEM((n_head, rows, HD), jnp.bfloat16),
                pltpu.VMEM((n_head, HD), jnp.float32),
                pltpu.VMEM((n_all, rows, HD), jnp.bfloat16),
                pltpu.VMEM((n_all, HD), jnp.float32),
                dma((n_head, 2, batch)),
                dma((2,)),
                dma((n_all,)),
                dma((n_all,)),
                dma((n_all,)),
                dma((n_all,)),
            ],
            compiler_params=pltpu.CompilerParams(collective_id=0, has_side_effects=True),
        )(lengths, block_map, query, key_cache, value_cache)
        return result

    placed = (
        P("grp", ("seq", "head"), None, None),
        P("grp", ("seq", "head"), None, None),
        P("grp", "head"),
        P("grp"),
        P("grp", None),
    )
    return jax.shard_map(
        on_device, mesh=mesh, in_specs=placed, out_specs=P("grp", "head"), check_vma=False
    )
```

```python
import functools

import jax
import jax.numpy as jnp
from jax import lax
from jax.experimental import pallas as pl
from jax.experimental.pallas import tpu as pltpu
from jax.sharding import PartitionSpec as P

QH = 32
KVH = 8
HD = 128
BLK = 128
REP = QH // KVH
MESH = pl.DeviceIdType.MESH
NEG = -1e30


def kernel(
    n_seq, n_head,
    lengths_hbm, map_hbm, q_hbm, k_hbm, v_hbm, out_ref,
    lengths, block_map, q_ref, small_sem,
    k_buf, v_buf, q_mate, num_send, stat_send, num_recv, stat_recv,
    kv_sem, q_sem, nsend_sem, nrecv_sem, ssend_sem, srecv_sem,
):
    seq = lax.axis_index("seq")
    head = lax.axis_index("head")
    batch, slots = k_hbm.shape[0], k_hbm.shape[1]
    width = k_hbm.shape[3] // n_head
    groups = width // HD
    rows_b = groups * REP
    rows = batch * rows_b
    tokens = slots * BLK
    me = seq * n_head + head
    n_all = n_seq * n_head
    small = n_all <= 16

    def loop(lo, hi, body):
        if small:
            for i in range(lo, hi):
                body(i)
        else:
            def step(i, carry):
                body(i)
                return carry
            lax.fori_loop(lo, hi, step, 0)

    def peer(step):
        return lax.rem(me + step, n_all)

    def place(device):
        return {"seq": device // n_head, "head": lax.rem(device, n_head)}

    barrier = pltpu.get_barrier_semaphore()

    def greet(step):
        pl.semaphore_signal(barrier, inc=1, device_id=place(peer(step)), device_id_type=MESH)

    smalls = [pltpu.make_async_copy(a, b, small_sem.at[i]) for i, (a, b) in enumerate(
        ((q_hbm, q_ref), (lengths_hbm, lengths), (map_hbm, block_map)))]
    for copy in smalls:
        copy.start()
    loop(1, n_all, greet)
    def load(half, which, b):
        owner = lax.rem(head + half, n_head)
        source, target = ((k_hbm, k_buf), (v_hbm, v_buf))[which]
        lanes = pl.ds(pl.multiple_of(owner * width, width), width)
        return pltpu.make_async_copy(
            source.at[b, :, :, lanes], target.at[half, b], kv_sem.at[half, which, b]
        )

    for half in range(n_head):
        for which in range(2):
            for b in range(batch):
                load(half, which, b).start()

    def live_of(b):
        flags = []
        for j in range(slots):
            here = block_map[b, me * slots + j] * BLK < lengths[b]
            flags.append(jnp.broadcast_to(jnp.where(here, 1.0, 0.0), (rows_b, BLK)))
        return jnp.concatenate(flags, axis=1) > 0.5

    def diagonal(q):
        lifted = q.astype(jnp.float32).reshape(rows, HD)
        wide = jnp.concatenate([lifted] * groups, axis=1)
        row_group = lax.rem(lax.broadcasted_iota(jnp.int32, wide.shape, 0), rows_b) // REP
        lane_group = lax.broadcasted_iota(jnp.int32, wide.shape, 1) // HD
        return jnp.where(row_group == lane_group, wide, 0.0).astype(jnp.bfloat16)

    for copy in smalls:
        copy.wait()
    live = [live_of(b) for b in range(batch)]

    def attend(half, q):
        spread = diagonal(q)
        expos, tops, totals, nums = [], [], [], []
        for b in range(batch):
            load(half, 0, b).wait()
        for b in range(batch):
            keys = k_buf[half, b].reshape(tokens, width)
            scores = lax.dot_general(
                spread[b * rows_b:(b + 1) * rows_b], keys, (((1,), (1,)), ((), ())),
                preferred_element_type=jnp.float32,
            ) * (1.0 / HD**0.5)
            scores = jnp.where(live[b], scores, NEG)
            top = jnp.max(scores, axis=1, keepdims=True)
            expo = jnp.where(live[b], jnp.exp(scores - top), 0.0)
            tops.append(top)
            totals.append(jnp.sum(expo, axis=1, keepdims=True))
            expos.append(expo.astype(jnp.bfloat16))
        for b in range(batch):
            load(half, 1, b).wait()
        for b in range(batch):
            values = v_buf[half, b].reshape(tokens, width)
            full = jnp.dot(expos[b], values, preferred_element_type=jnp.float32)
            row_group = lax.broadcasted_iota(jnp.int32, (rows_b, HD), 0) // REP
            part = jnp.zeros((rows_b, HD), jnp.float32)
            for g in range(groups):
                part = jnp.where(row_group == g, full[:, g * HD:(g + 1) * HD], part)
            nums.append(part)
        column = jnp.concatenate(tops + totals + [jnp.zeros((HD - 2 * rows, 1), jnp.float32)], axis=0)
        record = jnp.transpose(jnp.broadcast_to(column, (HD, HD)))[0:1]
        return jnp.concatenate(nums, axis=0), record

    def copies(device, half, slot_of):
        return (
            pltpu.make_async_remote_copy(
                src_ref=stat_send.at[pl.ds(half, 1)], dst_ref=stat_recv.at[pl.ds(slot_of, 1)],
                send_sem=ssend_sem.at[device], recv_sem=srecv_sem.at[slot_of],
                device_id=place(device), device_id_type=MESH,
            ),
            pltpu.make_async_remote_copy(
                src_ref=num_send.at[half], dst_ref=num_recv.at[slot_of],
                send_sem=nsend_sem.at[device], recv_sem=nrecv_sem.at[slot_of],
                device_id=place(device), device_id_type=MESH,
            ),
        )

    def send_half(half):
        def one(d):
            target_seq = lax.rem(seq + d, n_seq)
            target = target_seq * n_head + lax.rem(head + half, n_head)
            for copy in copies(target, half, me):
                copy.start()
        loop(0 if half else 1, n_seq, one)

    pl.semaphore_wait(barrier, n_all - 1)
    q_copy = pltpu.make_async_remote_copy(
        src_ref=q_ref, dst_ref=q_mate, send_sem=q_sem.at[0], recv_sem=q_sem.at[1],
        device_id={"head": lax.rem(head + 1, n_head)}, device_id_type=MESH,
    )
    q_copy.start()
    own_num, own_stat = attend(0, q_ref[...])
    num_send[0] = own_num.astype(jnp.bfloat16)
    stat_send[0:1] = own_stat
    send_half(0)
    q_copy.wait()
    mate_num, mate_stat = attend(1, q_mate[...])
    num_send[1] = mate_num.astype(jnp.bfloat16)
    stat_send[1:2] = mate_stat
    send_half(1)

    stat_recv[pl.ds(me, 1)] = own_stat
    num_recv[me] = own_num.astype(jnp.bfloat16)

    def arrive_stat(step):
        copies(peer(step), 0, peer(step))[0].wait_recv()

    def arrive_num(step):
        copies(peer(step), 0, peer(step))[1].wait_recv()

    loop(1, n_all, arrive_stat)
    stats = stat_recv[...]
    top = stats[:, :rows]
    total = stats[:, rows:2 * rows]
    factor = jnp.exp(top - jnp.max(top, axis=0, keepdims=True))
    share = factor / jnp.sum(factor * total, axis=0, keepdims=True)
    share_columns = jnp.transpose(jnp.concatenate(
        [share, jnp.zeros((n_all, HD - rows), jnp.float32)], axis=1))[:rows]
    loop(1, n_all, arrive_num)
    result = jnp.zeros((rows, HD), jnp.float32)
    for s in range(n_all):
        result = result + share_columns[:, s:s + 1] * num_recv[s].astype(jnp.float32)
    out_ref[...] = result.reshape(batch, rows_b * HD).astype(out_ref.dtype)

    def sent(step):
        for copy in copies(peer(step), 0, me):
            copy.wait_send()

    loop(1, n_all, sent)


def solution(mesh):
    n_seq, n_head = mesh.shape["seq"], mesh.shape["head"]
    n_all = n_seq * n_head

    def on_device(key_cache, value_cache, query, lengths, block_map):
        batch, slots, _, channels = key_cache.shape
        width = channels // n_head
        rows = batch * (width // HD) * REP
        dma = pltpu.SemaphoreType.DMA
        result = pl.pallas_call(
            functools.partial(kernel, n_seq, n_head),
            out_shape=pltpu.VMEM(query.shape, jnp.bfloat16),
            in_specs=[
                *[pl.BlockSpec(memory_space=pl.ANY)] * 5,
            ],
            out_specs=pl.BlockSpec(memory_space=pltpu.VMEM),
            scratch_shapes=[
                pltpu.SMEM(lengths.shape, jnp.int32),
                pltpu.SMEM(block_map.shape, jnp.int32),
                pltpu.VMEM(query.shape, jnp.bfloat16),
                dma((3,)),
                pltpu.VMEM((n_head, batch, slots, BLK, width), jnp.bfloat16),
                pltpu.VMEM((n_head, batch, slots, BLK, width), jnp.bfloat16),
                pltpu.VMEM(query.shape, jnp.bfloat16),
                pltpu.VMEM((n_head, rows, HD), jnp.bfloat16),
                pltpu.VMEM((n_head, HD), jnp.float32),
                pltpu.VMEM((n_all, rows, HD), jnp.bfloat16),
                pltpu.VMEM((n_all, HD), jnp.float32),
                dma((n_head, 2, batch)),
                dma((2,)),
                dma((n_all,)),
                dma((n_all,)),
                dma((n_all,)),
                dma((n_all,)),
            ],
            compiler_params=pltpu.CompilerParams(collective_id=0, has_side_effects=True),
        )(lengths, block_map, query, key_cache, value_cache)
        return result

    placed = (
        P("grp", ("seq", "head"), None, None),
        P("grp", ("seq", "head"), None, None),
        P("grp", "head"),
        P("grp"),
        P("grp", None),
    )
    return jax.shard_map(
        on_device, mesh=mesh, in_specs=placed, out_specs=P("grp", "head"), check_vma=False
    )
```

```python
import functools

import jax
import jax.numpy as jnp
from jax import lax
from jax.experimental import pallas as pl
from jax.experimental.pallas import tpu as pltpu
from jax.sharding import PartitionSpec as P

QH = 32
KVH = 8
HD = 128
BLK = 128
REP = QH // KVH
MESH = pl.DeviceIdType.MESH
NEG = -1e30


def kernel(
    n_seq, n_head,
    lengths_hbm, map_hbm, q_hbm, k_hbm, v_hbm, out_ref,
    lengths, block_map, q_ref, small_sem,
    k_buf, v_buf, q_mate, num_send, stat_send, num_recv, stat_recv,
    kv_sem, q_sem, nsend_sem, nrecv_sem, ssend_sem, srecv_sem,
):
    seq = lax.axis_index("seq")
    head = lax.axis_index("head")
    batch, slots = k_hbm.shape[0], k_hbm.shape[1]
    width = k_hbm.shape[3] // n_head
    groups = width // HD
    rows_b = groups * REP
    rows = batch * rows_b
    tokens = slots * BLK
    me = seq * n_head + head
    n_all = n_seq * n_head
    small = n_all <= 16

    def loop(lo, hi, body):
        if small:
            for i in range(lo, hi):
                body(i)
        else:
            def step(i, carry):
                body(i)
                return carry
            lax.fori_loop(lo, hi, step, 0)

    def peer(step):
        return lax.rem(me + step, n_all)

    def place(device):
        return {"seq": device // n_head, "head": lax.rem(device, n_head)}

    barrier = pltpu.get_barrier_semaphore()

    def greet(step):
        pl.semaphore_signal(barrier, inc=1, device_id=place(peer(step)), device_id_type=MESH)

    smalls = [pltpu.make_async_copy(a, b, small_sem.at[i]) for i, (a, b) in enumerate(
        ((q_hbm, q_ref), (lengths_hbm, lengths), (map_hbm, block_map)))]
    for copy in smalls:
        copy.start()
    loop(1, n_all, greet)
    def load(half, which, b):
        owner = lax.rem(head + half, n_head)
        source, target = ((k_hbm, k_buf), (v_hbm, v_buf))[which]
        lanes = pl.ds(pl.multiple_of(owner * width, width), width)
        return pltpu.make_async_copy(
            source.at[b, :, :, lanes], target.at[half, b], kv_sem.at[half, which, b]
        )

    for half in range(n_head):
        for which in range(2):
            for b in range(batch):
                load(half, which, b).start()

    def live_of(b):
        flags = []
        for j in range(slots):
            here = block_map[b, me * slots + j] * BLK < lengths[b]
            flags.append(jnp.broadcast_to(jnp.where(here, 1.0, 0.0), (rows_b, BLK)))
        return jnp.concatenate(flags, axis=1) > 0.5

    def diagonal(q):
        lifted = q.astype(jnp.float32).reshape(rows, HD)
        wide = jnp.concatenate([lifted] * groups, axis=1)
        row_group = lax.rem(lax.broadcasted_iota(jnp.int32, wide.shape, 0), rows_b) // REP
        lane_group = lax.broadcasted_iota(jnp.int32, wide.shape, 1) // HD
        return jnp.where(row_group == lane_group, wide, 0.0).astype(jnp.bfloat16)

    for copy in smalls:
        copy.wait()
    live = [live_of(b) for b in range(batch)]

    def attend(half, q):
        spread = diagonal(q)
        expos, tops, totals, nums = [], [], [], []
        if half == 0:
            for b in range(batch):
                load(half, 0, b).wait()
        for b in range(batch):
            keys = k_buf[half, b].reshape(tokens, width)
            scores = lax.dot_general(
                spread[b * rows_b:(b + 1) * rows_b], keys, (((1,), (1,)), ((), ())),
                preferred_element_type=jnp.float32,
            ) * (1.0 / HD**0.5)
            scores = jnp.where(live[b], scores, NEG)
            top = jnp.max(scores, axis=1, keepdims=True)
            expo = jnp.where(live[b], jnp.exp(scores - top), 0.0)
            tops.append(top)
            totals.append(jnp.sum(expo, axis=1, keepdims=True))
            expos.append(expo.astype(jnp.bfloat16))
        for b in range(batch):
            load(half, 1, b).wait()
            if half == 0:
                load(1, 0, b).wait()
        for b in range(batch):
            values = v_buf[half, b].reshape(tokens, width)
            full = jnp.dot(expos[b], values, preferred_element_type=jnp.float32)
            row_group = lax.broadcasted_iota(jnp.int32, (rows_b, HD), 0) // REP
            part = jnp.zeros((rows_b, HD), jnp.float32)
            for g in range(groups):
                part = jnp.where(row_group == g, full[:, g * HD:(g + 1) * HD], part)
            nums.append(part)
        column = jnp.concatenate(tops + totals, axis=0)
        record = jnp.transpose(jnp.broadcast_to(column, (2 * rows, HD)))[0:1]
        record = jnp.concatenate([record, jnp.zeros((1, HD - 2 * rows), jnp.float32)], axis=1)
        return jnp.concatenate(nums, axis=0), record

    def copies(device, half, slot_of):
        return (
            pltpu.make_async_remote_copy(
                src_ref=stat_send.at[pl.ds(half, 1)], dst_ref=stat_recv.at[pl.ds(slot_of, 1)],
                send_sem=ssend_sem.at[device], recv_sem=srecv_sem.at[slot_of],
                device_id=place(device), device_id_type=MESH,
            ),
            pltpu.make_async_remote_copy(
                src_ref=num_send.at[half], dst_ref=num_recv.at[slot_of],
                send_sem=nsend_sem.at[device], recv_sem=nrecv_sem.at[slot_of],
                device_id=place(device), device_id_type=MESH,
            ),
        )

    def send_half(half):
        def one(d):
            target_seq = lax.rem(seq + d, n_seq)
            target = target_seq * n_head + lax.rem(head + half, n_head)
            for copy in copies(target, half, me):
                copy.start()
        loop(0 if half else 1, n_seq, one)

    pl.semaphore_wait(barrier, n_all - 1)
    q_copy = pltpu.make_async_remote_copy(
        src_ref=q_ref, dst_ref=q_mate, send_sem=q_sem.at[0], recv_sem=q_sem.at[1],
        device_id={"head": lax.rem(head + 1, n_head)}, device_id_type=MESH,
    )
    q_copy.start()
    own_num, own_stat = attend(0, q_ref[...])
    num_send[0] = own_num.astype(jnp.bfloat16)
    stat_send[0:1] = own_stat
    send_half(0)
    q_copy.wait()
    mate_num, mate_stat = attend(1, q_mate[...])
    num_send[1] = mate_num.astype(jnp.bfloat16)
    stat_send[1:2] = mate_stat
    send_half(1)

    stat_recv[pl.ds(me, 1)] = own_stat
    num_recv[me] = own_num.astype(jnp.bfloat16)

    def arrive_stat(step):
        copies(peer(step), 0, peer(step))[0].wait_recv()

    def arrive_num(step):
        copies(peer(step), 0, peer(step))[1].wait_recv()

    loop(1, n_all, arrive_stat)
    stats = stat_recv[...]
    top = stats[:, :rows]
    total = stats[:, rows:2 * rows]
    factor = jnp.exp(top - jnp.max(top, axis=0, keepdims=True))
    share = factor / jnp.sum(factor * total, axis=0, keepdims=True)
    share_columns = jnp.transpose(jnp.concatenate(
        [share, jnp.zeros((n_all, HD - rows), jnp.float32)], axis=1))[:rows]
    loop(1, n_all, arrive_num)
    terms = [share_columns[:, s:s + 1] * num_recv[s].astype(jnp.float32) for s in range(n_all)]
    while len(terms) > 1:
        terms = [sum(terms[i + 1:i + 2], terms[i]) for i in range(0, len(terms), 2)]
    result = terms[0]
    out_ref[...] = result.reshape(batch, rows_b * HD).astype(out_ref.dtype)

    def sent(step):
        for copy in copies(peer(step), 0, me):
            copy.wait_send()

    loop(1, n_all, sent)


def solution(mesh):
    n_seq, n_head = mesh.shape["seq"], mesh.shape["head"]
    n_all = n_seq * n_head

    def on_device(key_cache, value_cache, query, lengths, block_map):
        batch, slots, _, channels = key_cache.shape
        width = channels // n_head
        rows = batch * (width // HD) * REP
        dma = pltpu.SemaphoreType.DMA
        result = pl.pallas_call(
            functools.partial(kernel, n_seq, n_head),
            out_shape=pltpu.VMEM(query.shape, jnp.bfloat16),
            in_specs=[
                *[pl.BlockSpec(memory_space=pl.ANY)] * 5,
            ],
            out_specs=pl.BlockSpec(memory_space=pltpu.VMEM),
            scratch_shapes=[
                pltpu.SMEM(lengths.shape, jnp.int32),
                pltpu.SMEM(block_map.shape, jnp.int32),
                pltpu.VMEM(query.shape, jnp.bfloat16),
                dma((3,)),
                pltpu.VMEM((n_head, batch, slots, BLK, width), jnp.bfloat16),
                pltpu.VMEM((n_head, batch, slots, BLK, width), jnp.bfloat16),
                pltpu.VMEM(query.shape, jnp.bfloat16),
                pltpu.VMEM((n_head, rows, HD), jnp.bfloat16),
                pltpu.VMEM((n_head, HD), jnp.float32),
                pltpu.VMEM((n_all, rows, HD), jnp.bfloat16),
                pltpu.VMEM((n_all, HD), jnp.float32),
                dma((n_head, 2, batch)),
                dma((2,)),
                dma((n_all,)),
                dma((n_all,)),
                dma((n_all,)),
                dma((n_all,)),
            ],
            compiler_params=pltpu.CompilerParams(collective_id=0, has_side_effects=True),
        )(lengths, block_map, query, key_cache, value_cache)
        return result

    placed = (
        P("grp", ("seq", "head"), None, None),
        P("grp", ("seq", "head"), None, None),
        P("grp", "head"),
        P("grp"),
        P("grp", None),
    )
    return jax.shard_map(
        on_device, mesh=mesh, in_specs=placed, out_specs=P("grp", "head"), check_vma=False
    )
```
